32 devices in a mesh: dp: 2 (over x), expert: 16 (over z, y, core).
Axes of the slice: x: 2, y: 2, z: 4, core: 2. Of those that a mesh axis runs over, the one named last changes fastest.
Arguments:
- grad_out: bfloat16 [4096, 2048], P(('dp', 'expert')), may hold values from -6 to 6
- expert_ids: int32 [4096, 6], P(('dp', 'expert')), may hold values from 0 to 15, all different within a row; in each aligned block of 128 rows (0 to 127, 128 to 255, ...) at most 64 rows name the same one
- gates: bfloat16 [4096, 6], P(('dp', 'expert')), may hold values from 0.049804688 to 1
- hidden: bfloat16 [32768, 704], P(('dp', 'expert')), may hold values from -6 to 6
- w_down: bfloat16 [16, 2048, 704], P('expert', 'dp'), may hold values from -0.21875 to 0.21875
Outputs:
- grad_hidden: bfloat16 [32768, 704], P(('dp', 'expert'))
- grad_down: float32 [16, 2048, 704], P('expert', 'dp')
- grad_gates: float32 [4096, 6], P(('dp', 'expert'))
The draws below stay inside these ranges and needn't reach their ends.
Inputs may be any that keep to these rules, and one draw needn't show every extreme that they name: `expert_ids`: in the rows of one device no expert is named by more than 64 rows; in every draw some device has an expert named by exactly 64 of its rows. A row names 6 different experts.
All inputs are finite; a program needn't handle non-finite values.
Results may differ from the reference program's by a relative error of at most 0.012.
Values may be sent and summed in bfloat16 or wider, within the bound.
A program may use at most 64 MiB of HBM per device.

```python
import math
import jax
import jax.numpy as jnp
import numpy as np
from jax import lax

D = 2048
FF_W = 704
TOP = 6
TOK_DEV = 128
EXPERTS = 16
CAP = 64
TOKENS = 4096
SLOTS = 32768
N_DP = 2
N_EXPERT = 16


def block_scale(rng, shape, split, low, top_value):
    def one(position, parts):
        draws = jax.random.uniform(jax.random.fold_in(jax.random.fold_in(rng, 6), position), (parts,), jnp.float32, low / len(split), top_value / len(split))
        return jnp.repeat(jnp.exp(draws), shape[position] // parts).reshape((-1,) + (1,) * (len(shape) - position - 1))

    gain = one(*split[0])
    for cut in split[1:]:
        gain = gain * one(*cut)
    return gain


def deal_out(rng, own, number, rows, amount, top, limit, lean):
    sequence = jax.random.permutation(rng, amount)
    crowded, ordinary = portions_of(amount, rows * top, limit, lean, True), portions_of(amount, rows * top, limit, lean, False)
    places = jnp.arange(amount)

    def named(sizes, rotation):
        used = int((sizes > 0).sum())
        fixed = max(1, used // 4)
        moved = fixed + (places - fixed + rotation * (used - fixed)) % max(1, amount - fixed)
        return jnp.zeros((amount,), jnp.int32).at[sequence[jnp.where(places < fixed, places, moved)]].set(jnp.asarray(sizes, jnp.int32))

    sizes = jnp.where(number % 4 == 0, named(crowded, number // 4), named(ordinary, number - number // 4 - 1))
    mixed = jax.random.permutation(jax.random.fold_in(own, 3), amount)
    source_of, taker = mixed[0:amount // 2 * 2:2], mixed[1:amount // 2 * 2:2]
    slack = jnp.minimum(sizes[source_of] - 1, limit - sizes[taker]) // 2
    slack = jnp.where((source_of == sequence[0]) | (taker == sequence[0]) | (sizes[taker] == 0), 0, jnp.maximum(slack, 0))
    moved = jax.random.randint(jax.random.fold_in(own, 4), (amount // 2,), 0, 1 << 20) % (slack + 1)
    sizes = sizes.at[source_of].add(-moved).at[taker].add(moved)
    members = jnp.searchsorted(jnp.cumsum(sizes), jnp.arange(rows * top), side="right").astype(jnp.int32)
    grid = members.reshape(top, rows).T
    grid = grid[jax.random.permutation(jax.random.fold_in(own, 1), rows)]
    rotation = jax.random.randint(jax.random.fold_in(own, 2), (rows, 1), 0, top)
    return jnp.take_along_axis(grid, (jnp.arange(top)[None, :] + rotation) % top, axis=1)


def portions_of(number_of, total, bound, lean, full):
    loads = [(1 << 20) // math.isqrt(rank ** lean) + 1 for rank in range(1, number_of + 1)]
    largest = bound if full else min(bound, max(-(-total // number_of), total * loads[0] // sum(loads)))
    least = 1 if total - largest >= number_of - 1 else 0
    counts, surplus = [largest] + [least] * (number_of - 1), total - largest - least * (number_of - 1)
    while surplus > 0:
        movable = [i for i in range(1, number_of) if counts[i] < largest] or [i for i in range(1, number_of) if counts[i] < bound]
        pool, remaining = sum([loads[i] for i in movable]), surplus
        for i in movable:
            extra = min(bound - counts[i], max(1, remaining * loads[i] // pool), surplus)
            counts[i] = counts[i] + extra
            surplus = surplus - extra
    return np.array(counts)


def bell_draw(own_key, extent, scale, limit, pieces=(), kind=jnp.bfloat16):
    drawn = jax.random.normal(own_key, extent, jnp.float32) * scale
    if len(pieces) > 0:
        drawn = block_scale(own_key, extent, pieces, -0.22, 0.18) * drawn
    return jnp.clip(drawn, min=-limit, max=limit).astype(kind)


def setup_inputs(seed: int = 0) -> dict:
    key_list = jax.random.split(jax.random.key(seed), 6)
    grad_out = bell_draw(key_list[0], (TOKENS, D), 1.0, 6.0, ((0, 32),))
    expert_ids_keys = jax.random.split(jax.random.fold_in(key_list[1], 1), TOKENS // TOK_DEV)
    expert_ids_turns = jax.random.permutation(jax.random.fold_in(key_list[1], 3), TOKENS // TOK_DEV)
    expert_ids = jax.vmap(lambda own, number: deal_out(jax.random.fold_in(key_list[1], 2), own, number, TOK_DEV, EXPERTS, TOP, CAP, 2))(expert_ids_keys, expert_ids_turns).reshape((TOKENS, TOP))
    gates = jnp.clip(0.049804688 + 0.9501953 * jax.random.uniform(key_list[2], (TOKENS, TOP), jnp.float32) ** block_scale(key_list[2], (TOKENS, TOP), ((0, 32),), -0.2, 0.2), 0.049804688, 1.0).astype(jnp.bfloat16)
    hidden = bell_draw(key_list[3], (SLOTS, FF_W), 1.0, 6.0, ((0, 32),))
    w_down = bell_draw(key_list[4], (EXPERTS, D, FF_W), FF_W ** -0.5, 0.21875, ((0, 16), (1, 2)))
    return dict(grad_out=grad_out, expert_ids=expert_ids, gates=gates, hidden=hidden, w_down=w_down)


def block_ranks(ids_flat):
    onehot = (ids_flat[:, :, None] == jnp.arange(N_EXPERT, dtype=jnp.int32)[None, None, :]).astype(jnp.int32)
    before = jnp.cumsum(onehot, axis=1) - onehot
    return jnp.sum(before * onehot, axis=2).astype(jnp.int32)


def reference(grad_out, expert_ids, gates, hidden, w_down):
    blocks = N_DP * N_EXPERT
    ids_flat = expert_ids.reshape(blocks, TOK_DEV * TOP)
    ranks = block_ranks(ids_flat)
    block_of = jnp.arange(blocks, dtype=jnp.int32)
    dp_of = block_of // N_EXPERT
    src_of = block_of % N_EXPERT
    flat_pos = ((dp_of[:, None] * N_EXPERT + ids_flat) * N_EXPERT + src_of[:, None]) * CAP + ranks
    tok_of = jnp.broadcast_to((jnp.arange(TOK_DEV * TOP, dtype=jnp.int32) // TOP)[None, :], flat_pos.shape)
    total = N_DP * N_EXPERT * N_EXPERT * CAP
    table_tok = jnp.zeros((total,), jnp.int32).at[flat_pos.reshape(-1)].set(tok_of.reshape(-1))
    table_gate = jnp.zeros((total,), jnp.bfloat16).at[flat_pos.reshape(-1)].set(gates.reshape(-1))
    table_live = jnp.zeros((total,), jnp.bfloat16).at[flat_pos.reshape(-1)].set(jnp.ones((blocks * TOK_DEV * TOP,), jnp.bfloat16))
    table_tok = table_tok.reshape(N_DP, N_EXPERT, N_EXPERT, CAP)
    table_gate = table_gate.reshape(N_DP, N_EXPERT, N_EXPERT * CAP)
    table_live = table_live.reshape(N_DP, N_EXPERT, N_EXPERT * CAP)
    dy_blocks = grad_out.reshape(N_DP, N_EXPERT, TOK_DEV, D)
    hid = hidden.reshape(N_DP, N_EXPERT, N_EXPERT * CAP, FF_W)

    def one_expert(e):
        weight = w_down[e]
        total_grad = jnp.zeros((D, FF_W), jnp.float32)
        hid_out = []
        slot_out = []
        for i in range(N_DP):
            toks = table_tok[i, e]
            rows = jax.vmap(lambda s, tk: dy_blocks[i, s][tk])(jnp.arange(N_EXPERT, dtype=jnp.int32), toks)
            rows = rows.reshape(N_EXPERT * CAP, D) * table_live[i, e][:, None]
            gate_row = table_gate[i, e].astype(jnp.float32)
            h_rows = hid[i, e]
            u = jnp.dot(rows, weight, preferred_element_type=jnp.float32)
            hid_out.append((gate_row[:, None] * u).astype(jnp.bfloat16))
            scaled = (gate_row[:, None] * rows.astype(jnp.float32)).astype(jnp.bfloat16)
            part = jnp.dot(scaled.T, h_rows, preferred_element_type=jnp.float32).astype(jnp.bfloat16)
            total_grad = total_grad + part.astype(jnp.float32)
            slot_out.append(jnp.sum(h_rows.astype(jnp.float32) * u, axis=1))
        return jnp.stack(hid_out), total_grad, jnp.stack(slot_out)

    grad_hid, grad_down, slot_grad = lax.map(one_expert, jnp.arange(N_EXPERT, dtype=jnp.int32))
    grad_hid = jnp.transpose(grad_hid, (1, 0, 2, 3)).reshape(total, FF_W)
    slot_grad = jnp.transpose(slot_grad, (1, 0, 2)).reshape(total)
    grad_gates = slot_grad[flat_pos.reshape(-1)].reshape(N_DP * N_EXPERT * TOK_DEV, TOP)
    return grad_hid, grad_down, grad_gates
```

```python
import functools

import jax
import jax.numpy as jnp
from jax import lax
from jax.experimental import pallas as pl
from jax.experimental.pallas import tpu as pltpu
from jax.sharding import PartitionSpec as P

LAG = 2
MESH = pl.DeviceIdType.MESH
F32 = jnp.float32
BF16 = jnp.bfloat16
NT = (((1,), (1,)), ((), ()))


def kernel(
    n, dp, cap,
    ids_ref, gates_ref, x_ref, h_ref, w_ref,
    gh_ref, gd_ref, gg_ref,
    gbuf, xs, wt, ht, hg, gh, gd, psend, precv, meta_send, meta_recv, sel, pad, grow, sg, ggs, ggr,
    loc_sem, ring_ss, ring_rs, d2d_ss, d2d_rs, own_ss, own_rs, w_ss, w_rs, meta_ss, meta_rs,
    p_ss, p_rs, gg_ss, gg_rs,
):
    me = lax.axis_index("expert")
    di = lax.axis_index("dp")
    ring = n // 2
    half_ring = ring // 2
    side = n // 4
    top, tok = ids_ref.shape
    width = x_ref.shape[1] // dp
    slots = h_ref.shape[1]
    core = lax.rem(me, 2)
    mate = me + 1 - 2 * core
    bit = lax.rem(me // 2, 2)
    pos = me // 4 + bit * (ring - 1 - 2 * (me // 4))

    def at(position, c):
        q = lax.rem(position + ring, ring)
        b = q // side
        return ((q + b * (ring - 1 - 2 * q)) * 2 + b) * 2 + c

    ahead = (at(pos + 1, core), at(pos - 1, core))
    half = tok // 2

    barrier = pltpu.get_barrier_semaphore()

    @pl.loop(1, n)
    def _(j):
        pl.semaphore_signal(barrier, 1, device_id={"expert": lax.rem(me + j, n)}, device_id_type=MESH)

    for j in range(1, dp):
        pl.semaphore_signal(barrier, 1, device_id={"dp": lax.rem(di + j, dp)}, device_id_type=MESH)

    chunk_id = [lax.rem(di + 1 + j, dp) for j in range(dp)]

    def x_cols(j):
        return x_ref.at[:, pl.ds(pl.multiple_of(chunk_id[j] * width, width), width)]

    local = [pltpu.make_async_copy(x_cols(j), gbuf.at[j, me], loc_sem.at[j]) for j in range(dp)]
    h_copy = pltpu.make_async_copy(h_ref, ht, loc_sem.at[dp])
    w_copy = pltpu.make_async_copy(w_ref, wt.at[di], loc_sem.at[dp + 1])
    for copy in local + [h_copy, w_copy]:
        copy.start()

    expert_row = lax.broadcasted_iota(jnp.int32, (n, tok), 0)
    hit = jnp.zeros((n, tok), F32)
    gate = jnp.zeros((n, tok), F32)
    gates = gates_ref[...].astype(F32)
    for k in range(top):
        same = ids_ref[k : k + 1, :] == expert_row
        hit = hit + jnp.where(same, 1.0, 0.0)
        gate = gate + jnp.where(same, gates[k : k + 1, :], 0.0)
    before = lax.broadcasted_iota(jnp.int32, (tok, tok), 0) < lax.broadcasted_iota(jnp.int32, (tok, tok), 1)
    rank = jnp.dot(hit.astype(BF16), jnp.where(before, 1.0, 0.0).astype(BF16), preferred_element_type=F32)
    rank = jnp.where(hit > 0.5, rank, -1.0)
    for e in range(n):
        meta_send[e, 0:1, :] = rank[e : e + 1, :]
        meta_send[e, 1:2, :] = gate[e : e + 1, :]
        meta_send[e, 2:8, :] = jnp.zeros((6, tok), F32)

    pl.semaphore_wait(barrier, n - 1 + dp - 1)

    def remote(src, dst, ss, rs, **where):
        return pltpu.make_async_remote_copy(
            src_ref=src, dst_ref=dst, send_sem=ss, recv_sem=rs, device_id=where, device_id_type=MESH
        )

    def w_send(j):
        return remote(w_ref, wt.at[di], w_ss.at[j], w_rs.at[j], dp=lax.rem(di + j, dp))

    def w_recv(j):
        return remote(w_ref, wt.at[lax.rem(di + dp - j, dp)], w_ss.at[j], w_rs.at[j], dp=lax.rem(di + j, dp))

    def rows_of(step, d):
        if step < half_ring:
            return pl.ds(0, tok)
        return pl.ds(d * half, half)

    def ring_send(j, d, step):
        owner = at(pos - (step - 1) * (1 - 2 * d), core)
        rows = rows_of(step, d)
        if step == 1:
            src = x_ref.at[rows, pl.ds(pl.multiple_of(chunk_id[j] * width, width), width)]
        else:
            src = gbuf.at[j, owner, rows]
        return remote(
            src, gbuf.at[j, owner, rows], ring_ss.at[j, d, step - 1], ring_rs.at[j, d, step - 1],
            expert=ahead[d],
        )

    def ring_recv(j, d, step):
        owner = at(pos - step * (1 - 2 * d), core)
        rows = rows_of(step, d)
        return remote(
            gbuf.at[j, owner, rows], gbuf.at[j, owner, rows],
            ring_ss.at[j, d, step - 1], ring_rs.at[j, d, step - 1], expert=ahead[d],
        )

    def pass_on(j, d, step, c):
        owner = at(pos - step * (1 - 2 * d), c)
        rows = rows_of(step, d)
        return remote(
            gbuf.at[j, owner, rows], gbuf.at[j, owner, rows],
            d2d_ss.at[j, d, step - 1], d2d_rs.at[j, d, step - 1], expert=mate,
        )

    def own_send(j):
        return remote(x_cols(j), gbuf.at[j, me], own_ss.at[j], own_rs.at[j], expert=mate)

    def own_recv(j):
        return remote(x_cols(j), gbuf.at[j, mate], own_ss.at[j], own_rs.at[j], expert=mate)

    def meta_copy(j, e):
        return remote(
            meta_send.at[lax.rem(me + j, n)], meta_recv.at[e],
            meta_ss.at[j], meta_rs.at[j], expert=lax.rem(me + j, n),
        )

    for d in range(2):
        ring_send(0, d, 1).start()

    @pl.loop(1, n)
    def _(j):
        meta_copy(j, me).start()

    for j in range(1, dp):
        w_send(j).start()
    own_send(0).start()
    meta_local = pltpu.make_async_copy(meta_send.at[me], meta_recv.at[me], loc_sem.at[dp + 2])
    meta_local.start()
    meta_local.wait()

    @pl.loop(1, n)
    def _(j):
        meta_copy(j, lax.rem(me + n - j, n)).wait_recv()

    group = tok // cap
    slot_row = lax.broadcasted_iota(jnp.int32, (cap, tok), 0).astype(F32)
    slot_wide = lax.broadcasted_iota(jnp.int32, (tok, tok), 0).astype(F32)
    for g in range(n // group):
        total = jnp.zeros((8, tok), F32)
        for m in range(group):
            e = g * group + m
            where = meta_recv[e, 0:1, :]
            sel[e] = jnp.where(where == slot_row, 1.0, 0.0).astype(BF16)
            shifted = jnp.where(where < 0.0, -1.0, where + float(m * cap))
            wide = jnp.where(shifted == slot_wide, 1.0, 0.0)
            pad[e] = wide
            amount = jnp.broadcast_to(meta_recv[e, 1:2, :], (8, tok)).astype(BF16)
            total = total + lax.dot_general(amount, wide.astype(BF16), NT, preferred_element_type=F32)
        grow[:, g * tok : (g + 1) * tok] = total

    h_copy.wait()
    hg[...] = (ht[...].astype(F32) * grow[0:1, :]).astype(BF16)

    def pick(j, e):
        out = jnp.dot(sel[e], gbuf[j, e], preferred_element_type=F32)
        xs[j, pl.ds(pl.multiple_of(e * cap, cap), cap), :] = out.astype(BF16)

    tile = min(256, width)

    def share(j, place):
        @pl.loop(0, width // tile)
        def _(m):
            cols = pl.ds(pl.multiple_of(m * tile, tile), tile)
            place(m, cols, jnp.dot(hg[...], xs[j, :, cols], preferred_element_type=F32))

    def p_copy(j):
        return remote(psend.at[j], precv.at[j], p_ss.at[j], p_rs.at[j], dp=chunk_id[j])

    def put_send(j):
        def place(m, cols, value):
            psend[j, :, cols] = value.astype(BF16)

        return place

    def put_own(m, cols, value):
        gd[:, cols] = value.astype(BF16).astype(F32)

    def finish(j):
        if j < dp - 1:
            share(j, put_send(j))
            p_copy(j).start()
        else:
            share(j, put_own)

    for j in range(dp):
        local[j].wait()
    pick(0, me)
    own_recv(0).wait_recv()
    pick(0, mate)

    last = half_ring + LAG * (dp - 1)
    mates = []
    for t in range(1, last + 2):
        fresh, done = [], []
        for j in range(dp):
            s = t - LAG * j
            if s == 0:
                for d in range(2):
                    ring_send(j, d, 1).start()
                own_send(j).start()
            if 1 <= s <= half_ring:
                for d in range(2):
                    ring_recv(j, d, s).wait_recv()
                    if s < half_ring:
                        ring_send(j, d, s + 1).start()
                    pass_on(j, d, s, core).start()
                    if s < half_ring or d == 1:
                        fresh.append((j, at(pos - s * (1 - 2 * d), core)))
        for j, e in fresh:
            pick(j, e)
        for j in range(dp):
            s = t - 1 - LAG * j
            if s == 0 and j > 0:
                pick(j, me)
                own_recv(j).wait_recv()
                pick(j, mate)
            if 1 <= s <= half_ring:
                for d in range(2):
                    pass_on(j, d, s, 1 - core).wait_recv()
                    if s < half_ring or d == 1:
                        pick(j, at(pos - s * (1 - 2 * d), 1 - core))
            if s == half_ring:
                finish(j)

    w_copy.wait()
    for j in range(1, dp):
        w_recv(j).wait_recv()

    step = min(256, slots)

    @pl.loop(0, slots // step)
    def _(m):
        rows = pl.ds(pl.multiple_of(m * step, step), step)
        ut = lax.dot_general(wt[chunk_id[0]], xs[0, rows, :], NT, preferred_element_type=F32)
        for j in range(1, dp):
            ut = ut + lax.dot_general(wt[chunk_id[j]], xs[j, rows, :], NT, preferred_element_type=F32)
        gh[:, rows] = (ut * grow[0:1, rows]).astype(BF16)
        total = jnp.sum(ht[:, rows].astype(F32) * ut, axis=0, keepdims=True)
        sg[:, rows] = jnp.broadcast_to(total, (8, step))

    gh_out = pltpu.make_async_copy(gh, gh_ref, loc_sem.at[dp + 3])
    for e in range(n):
        g = e // group
        ggs[e] = jnp.dot(
            sg[:, g * tok : (g + 1) * tok], pad[e], precision=lax.Precision.HIGHEST,
            preferred_element_type=F32,
        )
    gh_out.start()

    def gg_copy(j, e):
        return remote(
            ggs.at[lax.rem(me + j, n)], ggr.at[e], gg_ss.at[j], gg_rs.at[j], expert=lax.rem(me + j, n)
        )

    @pl.loop(1, n)
    def _(j):
        gg_copy(j, me).start()

    gg_local = pltpu.make_async_copy(ggs.at[me], ggr.at[me], loc_sem.at[dp + 2])
    gg_local.start()
    gg_local.wait()

    @pl.loop(1, n)
    def _(j):
        gg_copy(j, lax.rem(me + n - j, n)).wait_recv()

    back = jnp.zeros((top, tok), F32)
    for e in range(n):
        back = back + jnp.where(ids_ref[...] == e, ggr[e, 0:1, :], 0.0)
    gg_ref[...] = back

    for j in range(dp - 1):
        p_copy(j).wait_recv()

    gd_out = []
    for m in range(width // tile):
        cols = slice(m * tile, (m + 1) * tile)
        value = gd[:, cols]
        for j in range(dp - 1):
            value = value + precv[j, :, cols].astype(F32)
        gd[:, cols] = value
        if m > 0:
            gd_out[-1].start()
        gd_out.append(pltpu.make_async_copy(
            gd.at[:, pl.ds(m * tile, tile)], gd_ref.at[:, pl.ds(m * tile, tile)], loc_sem.at[dp + 4 + m]
        ))
    gd_out[-1].start()

    for j in range(dp):
        own_send(j).wait_send()
        for d in range(2):
            for s in range(1, half_ring + 1):
                ring_send(j, d, s).wait_send()
                pass_on(j, d, s, core).wait_send()
    for j in range(1, dp):
        w_send(j).wait_send()
        p_copy(j - 1).wait_send()

    @pl.loop(1, n)
    def _(j):
        meta_copy(j, me).wait_send()
        gg_copy(j, me).wait_send()

    gh_out.wait()
    for copy in gd_out:
        copy.wait()


def shards(n, dp, grad_out, expert_ids, gates, hidden, w_down):
    tok, depth = grad_out.shape
    top = expert_ids.shape[1]
    slots, units = hidden.shape
    cap = slots // n
    width = depth // dp
    steps = n // 4
    tiles = width // min(256, width)
    any_spec = pl.BlockSpec(memory_space=pl.ANY)
    vmem_spec = pl.BlockSpec(memory_space=pltpu.VMEM)
    dma = pltpu.SemaphoreType.DMA
    gh, gd, gg = pl.pallas_call(
        functools.partial(kernel, n, dp, cap),
        out_shape=(
            jax.ShapeDtypeStruct((units, slots), BF16),
            jax.ShapeDtypeStruct((units, width), F32),
            jax.ShapeDtypeStruct((top, tok), F32),
        ),
        in_specs=[vmem_spec, vmem_spec, any_spec, any_spec, any_spec],
        out_specs=(any_spec, any_spec, vmem_spec),
        scratch_shapes=[
            pltpu.VMEM((dp, n, tok, width), BF16),
            pltpu.VMEM((dp, slots, width), BF16),
            pltpu.VMEM((dp, units, width), BF16),
            pltpu.VMEM((units, slots), BF16),
            pltpu.VMEM((units, slots), BF16),
            pltpu.VMEM((units, slots), BF16),
            pltpu.VMEM((units, width), F32),
            pltpu.VMEM((dp - 1, units, width), BF16),
            pltpu.VMEM((dp - 1, units, width), BF16),
            pltpu.VMEM((n, 8, tok), F32),
            pltpu.VMEM((n, 8, tok), F32),
            pltpu.VMEM((n, cap, tok), BF16),
            pltpu.VMEM((n, tok, tok), F32),
            pltpu.VMEM((8, slots), F32),
            pltpu.VMEM((8, slots), F32),
            pltpu.VMEM((n, 8, tok), F32),
            pltpu.VMEM((n, 8, tok), F32),
            dma((dp + 4 + tiles,)),
            dma((dp, 2, steps)),
            dma((dp, 2, steps)),
            dma((dp, 2, steps)),
            dma((dp, 2, steps)),
            dma((dp,)),
            dma((dp,)),
            dma((dp,)),
            dma((dp,)),
            dma((n,)),
            dma((n,)),
            dma((dp,)),
            dma((dp,)),
            dma((n,)),
            dma((n,)),
        ],
        compiler_params=pltpu.CompilerParams(
            collective_id=0, has_side_effects=True, vmem_limit_bytes=64_000_000
        ),
    )(expert_ids.T, gates.T, grad_out, hidden.T, w_down[0].T)
    return gh.T, gd.T[None], gg.T


def solution(mesh):
    n, dp = mesh.shape["expert"], mesh.shape["dp"]
    return jax.shard_map(
        functools.partial(shards, n, dp),
        mesh=mesh,
        in_specs=(
            P(("dp", "expert"), None),
            P(("dp", "expert"), None),
            P(("dp", "expert"), None),
            P(("dp", "expert"), None),
            P("expert", "dp", None),
        ),
        out_specs=(P(("dp", "expert"), None), P("expert", "dp", None), P(("dp", "expert"), None)),
        check_vma=False,
    )
```

```python
import functools

import jax
import jax.numpy as jnp
from jax import lax
from jax.experimental import pallas as pl
from jax.experimental.pallas import tpu as pltpu
from jax.sharding import PartitionSpec as P

LAG = 2
SUB = 2
MESH = pl.DeviceIdType.MESH
F32 = jnp.float32
BF16 = jnp.bfloat16
NT = (((1,), (1,)), ((), ()))


def kernel(
    n, dp, cap,
    ids_ref, gates_ref, x_ref, h_ref, w_ref,
    gh_ref, gd_ref, gg_ref,
    gbuf, xs, wt, ht, hg, ua, psend, precv, meta_send, meta_recv, sel, pad, grow, sg, ggs, ggr,
    loc_sem, ring_ss, ring_rs, d2d_ss, d2d_rs, own_ss, own_rs, w_ss, w_rs, meta_ss, meta_rs,
    p_ss, p_rs, gg_ss, gg_rs,
):
    me = lax.axis_index("expert")
    di = lax.axis_index("dp")
    ring = n // 2
    half_ring = ring // 2
    side = n // 4
    top, tok = ids_ref.shape
    width = x_ref.shape[1] // dp
    piece = width // SUB
    parts = dp * SUB
    slots = h_ref.shape[1]
    core = lax.rem(me, 2)
    mate = me + 1 - 2 * core
    bit = lax.rem(me // 2, 2)
    pos = me // 4 + bit * (ring - 1 - 2 * (me // 4))

    def at(position, c):
        q = lax.rem(position + ring, ring)
        b = q // side
        return ((q + b * (ring - 1 - 2 * q)) * 2 + b) * 2 + c

    ahead = (at(pos + 1, core), at(pos - 1, core))
    half = tok // 2

    barrier = pltpu.get_barrier_semaphore()

    @pl.loop(1, n)
    def _(j):
        pl.semaphore_signal(barrier, 1, device_id={"expert": lax.rem(me + j, n)}, device_id_type=MESH)

    for j in range(1, dp):
        pl.semaphore_signal(barrier, 1, device_id={"dp": lax.rem(di + j, dp)}, device_id_type=MESH)

    owner_of = [lax.rem(di + 1 + j // SUB, dp) for j in range(parts)]

    def span(j):
        return pl.ds(pl.multiple_of(owner_of[j] * width + (j % SUB) * piece, piece), piece)

    def x_cols(j):
        return x_ref.at[:, span(j)]

    local = [pltpu.make_async_copy(x_cols(j), gbuf.at[j, me], loc_sem.at[j]) for j in range(parts)]
    h_copy = pltpu.make_async_copy(h_ref, ht, loc_sem.at[parts])
    w_copy = pltpu.make_async_copy(w_ref, wt.at[di], loc_sem.at[parts + 1])
    for copy in local + [h_copy, w_copy]:
        copy.start()

    expert_row = lax.broadcasted_iota(jnp.int32, (n, tok), 0)
    hit = jnp.zeros((n, tok), F32)
    gate = jnp.zeros((n, tok), F32)
    gates = gates_ref[...].astype(F32)
    for k in range(top):
        same = ids_ref[k : k + 1, :] == expert_row
        hit = hit + jnp.where(same, 1.0, 0.0)
        gate = gate + jnp.where(same, gates[k : k + 1, :], 0.0)
    before = lax.broadcasted_iota(jnp.int32, (tok, tok), 0) < lax.broadcasted_iota(jnp.int32, (tok, tok), 1)
    rank = jnp.dot(hit.astype(BF16), jnp.where(before, 1.0, 0.0).astype(BF16), preferred_element_type=F32)
    rank = jnp.where(hit > 0.5, rank, -1.0)
    for e in range(n):
        meta_send[e, 0:1, :] = rank[e : e + 1, :]
        meta_send[e, 1:2, :] = gate[e : e + 1, :]
        meta_send[e, 2:8, :] = jnp.zeros((6, tok), F32)

    pl.semaphore_wait(barrier, n - 1 + dp - 1)

    def remote(src, dst, ss, rs, **where):
        return pltpu.make_async_remote_copy(
            src_ref=src, dst_ref=dst, send_sem=ss, recv_sem=rs, device_id=where, device_id_type=MESH
        )

    def w_send(j):
        return remote(w_ref, wt.at[di], w_ss.at[j], w_rs.at[j], dp=lax.rem(di + j, dp))

    def w_recv(j):
        return remote(w_ref, wt.at[lax.rem(di + dp - j, dp)], w_ss.at[j], w_rs.at[j], dp=lax.rem(di + j, dp))

    def rows_of(step, d):
        if step < half_ring:
            return pl.ds(0, tok)
        return pl.ds(d * half, half)

    def ring_send(j, d, step):
        owner = at(pos - (step - 1) * (1 - 2 * d), core)
        rows = rows_of(step, d)
        if step == 1:
            src = x_ref.at[rows, span(j)]
        else:
            src = gbuf.at[j, owner, rows]
        return remote(
            src, gbuf.at[j, owner, rows], ring_ss.at[j, d, step - 1], ring_rs.at[j, d, step - 1],
            expert=ahead[d],
        )

    def ring_recv(j, d, step):
        owner = at(pos - step * (1 - 2 * d), core)
        rows = rows_of(step, d)
        return remote(
            gbuf.at[j, owner, rows], gbuf.at[j, owner, rows],
            ring_ss.at[j, d, step - 1], ring_rs.at[j, d, step - 1], expert=ahead[d],
        )

    def pass_on(j, d, step, c):
        owner = at(pos - step * (1 - 2 * d), c)
        rows = rows_of(step, d)
        return remote(
            gbuf.at[j, owner, rows], gbuf.at[j, owner, rows],
            d2d_ss.at[j, d, step - 1], d2d_rs.at[j, d, step - 1], expert=mate,
        )

    def own_send(j):
        return remote(x_cols(j), gbuf.at[j, me], own_ss.at[j], own_rs.at[j], expert=mate)

    def own_recv(j):
        return remote(x_cols(j), gbuf.at[j, mate], own_ss.at[j], own_rs.at[j], expert=mate)

    def meta_copy(j, e):
        return remote(
            meta_send.at[lax.rem(me + j, n)], meta_recv.at[e],
            meta_ss.at[j], meta_rs.at[j], expert=lax.rem(me + j, n),
        )

    for j in range(1, dp):
        w_send(j).start()
    for d in range(2):
        ring_send(0, d, 1).start()

    @pl.loop(1, n)
    def _(j):
        meta_copy(j, me).start()

    own_send(0).start()
    meta_local = pltpu.make_async_copy(meta_send.at[me], meta_recv.at[me], loc_sem.at[parts + 2])
    meta_local.start()
    meta_local.wait()

    @pl.loop(1, n)
    def _(j):
        meta_copy(j, lax.rem(me + n - j, n)).wait_recv()

    group = tok // cap
    slot_row = lax.broadcasted_iota(jnp.int32, (cap, tok), 0).astype(F32)
    slot_wide = lax.broadcasted_iota(jnp.int32, (tok, tok), 0).astype(F32)
    for g in range(n // group):
        total = jnp.zeros((8, tok), F32)
        for m in range(group):
            e = g * group + m
            where = meta_recv[e, 0:1, :]
            sel[e] = jnp.where(where == slot_row, 1.0, 0.0).astype(BF16)
            shifted = jnp.where(where < 0.0, -1.0, where + float(m * cap))
            wide = jnp.where(shifted == slot_wide, 1.0, 0.0)
            pad[e] = wide
            amount = jnp.broadcast_to(meta_recv[e, 1:2, :], (8, tok)).astype(BF16)
            total = total + lax.dot_general(amount, wide.astype(BF16), NT, preferred_element_type=F32)
        grow[:, g * tok : (g + 1) * tok] = total

    h_copy.wait()
    hg[...] = (ht[...].astype(F32) * grow[0:1, :]).astype(BF16)

    def pick(j, e):
        out = jnp.dot(sel[e], gbuf[j, e], preferred_element_type=F32)
        xs[j, pl.ds(pl.multiple_of(e * cap, cap), cap), :] = out.astype(BF16)

    tile = min(256, piece)

    def share(j, place):
        @pl.loop(0, piece // tile)
        def _(m):
            cols = pl.ds(pl.multiple_of(m * tile, tile), tile)
            place(m, cols, jnp.dot(hg[...], xs[j, :, cols], preferred_element_type=F32))

    def p_copy(j):
        return remote(psend.at[j], precv.at[j], p_ss.at[j], p_rs.at[j], dp=owner_of[j])

    def put_send(j):
        def place(m, cols, value):
            psend[j, :, cols] = value.astype(BF16)

        return place

    def put_own(j):
        def place(m, cols, value):
            to = pl.ds(pl.multiple_of((j % SUB) * piece + m * tile, tile), tile)
            gd_ref[:, to] = value.astype(BF16).astype(F32)

        return place

    def finish(j):
        if j < parts - SUB:
            share(j, put_send(j))
            p_copy(j).start()
        else:
            share(j, put_own(j))

    for j in range(parts):
        local[j].wait()
    pick(0, me)
    own_recv(0).wait_recv()
    pick(0, mate)

    step = min(256, slots)

    def product(j, rows):
        part = wt[owner_of[j], :, (j % SUB) * piece : (j % SUB + 1) * piece]
        return lax.dot_general(part, xs[j, rows, :], NT, preferred_element_type=F32)

    last = half_ring + LAG * (parts - 1)
    for t in range(1, last + 1):
        fresh = []
        if t == last:
            w_copy.wait()
            for j in range(1, dp):
                w_recv(j).wait_recv()

            @pl.loop(0, slots // step)
            def _(m):
                rows = pl.ds(pl.multiple_of(m * step, step), step)
                early = product(0, rows)
                for j in range(1, parts - 1):
                    early = early + product(j, rows)
                ua[:, rows] = early

        for j in range(parts):
            s = t - LAG * j
            if s == 0:
                for d in range(2):
                    ring_send(j, d, 1).start()
                own_send(j).start()
            if 1 <= s <= half_ring:
                for d in range(2):
                    ring_recv(j, d, s).wait_recv()
                    if s < half_ring:
                        ring_send(j, d, s + 1).start()
                    pass_on(j, d, s, core).start()
                    if s < half_ring or d == 1:
                        fresh.append((j, at(pos - s * (1 - 2 * d), core)))
        for j, e in fresh:
            pick(j, e)
        for j in range(parts):
            s = t - LAG * j
            if s == 1 and j > 0:
                pick(j, me)
                own_recv(j).wait_recv()
                pick(j, mate)
            if s < 1 or s > half_ring:
                continue
            for q in [s - 1] + [s] * (s == half_ring):
                for d in range(2 if q > 0 else 0):
                    pass_on(j, d, q, 1 - core).wait_recv()
                    if q < half_ring or d == 1:
                        pick(j, at(pos - q * (1 - 2 * d), 1 - core))
            if s == half_ring:
                finish(j)


    @pl.loop(0, slots // step)
    def _(m):
        rows = pl.ds(pl.multiple_of(m * step, step), step)
        ut = ua[:, rows] + product(parts - 1, rows)
        gh_ref[:, rows] = (ut * grow[0:1, rows]).astype(BF16)
        total = jnp.sum(ht[:, rows].astype(F32) * ut, axis=0, keepdims=True)
        sg[:, rows] = jnp.broadcast_to(total, (8, step))

    for e in range(n):
        g = e // group
        ggs[e] = jnp.dot(
            sg[:, g * tok : (g + 1) * tok], pad[e], precision=lax.Precision.HIGHEST,
            preferred_element_type=F32,
        )

    def gg_copy(j, e):
        return remote(
            ggs.at[lax.rem(me + j, n)], ggr.at[e], gg_ss.at[j], gg_rs.at[j], expert=lax.rem(me + j, n)
        )

    @pl.loop(1, n)
    def _(j):
        gg_copy(j, me).start()

    gg_local = pltpu.make_async_copy(ggs.at[me], ggr.at[me], loc_sem.at[parts + 2])
    gg_local.start()
    gg_local.wait()

    @pl.loop(1, n)
    def _(j):
        gg_copy(j, lax.rem(me + n - j, n)).wait_recv()

    back = jnp.zeros((top, tok), F32)
    for e in range(n):
        back = back + jnp.where(ids_ref[...] == e, ggr[e, 0:1, :], 0.0)
    gg_ref[...] = back

    for q in range(SUB):
        for j in range(q, parts - SUB, SUB):
            p_copy(j).wait_recv()
            cols = slice(q * piece, (q + 1) * piece)
            gd_ref[:, cols] = gd_ref[:, cols] + precv[j].astype(F32)

    for j in range(parts):
        own_send(j).wait_send()
        for d in range(2):
            for s in range(1, half_ring + 1):
                ring_send(j, d, s).wait_send()
                pass_on(j, d, s, core).wait_send()
    for j in range(1, dp):
        w_send(j).wait_send()
    for j in range(parts - SUB):
        p_copy(j).wait_send()

    @pl.loop(1, n)
    def _(j):
        meta_copy(j, me).wait_send()
        gg_copy(j, me).wait_send()


def shards(n, dp, grad_out, expert_ids, gates, hidden, w_down):
    tok, depth = grad_out.shape
    top = expert_ids.shape[1]
    slots, units = hidden.shape
    cap = slots // n
    width = depth // dp
    steps = n // 4
    parts, piece = dp * SUB, width // SUB
    held = 2 * (depth * (n * tok + slots) + units * (depth + 4 * slots + 2 * depth))
    held += 4 * n * tok * (tok + 40) + 2 * n * cap * tok + 64 * slots
    any_spec = pl.BlockSpec(memory_space=pltpu.HBM)
    vmem_spec = pl.BlockSpec(memory_space=pltpu.VMEM)
    dma = pltpu.SemaphoreType.DMA
    gh, gd, gg = pl.pallas_call(
        functools.partial(kernel, n, dp, cap),
        out_shape=(
            pltpu.VMEM((units, slots), BF16),
            pltpu.VMEM((units, width), F32),
            jax.ShapeDtypeStruct((top, tok), F32),
        ),
        in_specs=[vmem_spec, vmem_spec, any_spec, any_spec, any_spec],
        out_specs=(vmem_spec, vmem_spec, vmem_spec),
        scratch_shapes=[
            pltpu.VMEM((parts, n, tok, piece), BF16),
            pltpu.VMEM((parts, slots, piece), BF16),
            pltpu.VMEM((dp, units, width), BF16),
            pltpu.VMEM((units, slots), BF16),
            pltpu.VMEM((units, slots), BF16),
            pltpu.VMEM((units, slots), F32),
            pltpu.VMEM((parts - SUB, units, piece), BF16),
            pltpu.VMEM((parts - SUB, units, piece), BF16),
            pltpu.VMEM((n, 8, tok), F32),
            pltpu.VMEM((n, 8, tok), F32),
            pltpu.VMEM((n, cap, tok), BF16),
            pltpu.VMEM((n, tok, tok), F32),
            pltpu.VMEM((8, slots), F32),
            pltpu.VMEM((8, slots), F32),
            pltpu.VMEM((n, 8, tok), F32),
            pltpu.VMEM((n, 8, tok), F32),
            dma((parts + 3,)),
            dma((parts, 2, steps)),
            dma((parts, 2, steps)),
            dma((parts, 2, steps)),
            dma((parts, 2, steps)),
            dma((parts,)),
            dma((parts,)),
            dma((dp,)),
            dma((dp,)),
            dma((n,)),
            dma((n,)),
            dma((parts,)),
            dma((parts,)),
            dma((n,)),
            dma((n,)),
        ],
        compiler_params=pltpu.CompilerParams(
            collective_id=0, has_side_effects=True, vmem_limit_bytes=min(held + 6_000_000, 64_000_000)
        ),
    )(expert_ids.T, gates.T, grad_out, hidden.T, w_down[0].T)
    return gh.T, gd.T[None], gg.T


def solution(mesh):
    n, dp = mesh.shape["expert"], mesh.shape["dp"]
    return jax.shard_map(
        functools.partial(shards, n, dp),
        mesh=mesh,
        in_specs=(
            P(("dp", "expert"), None),
            P(("dp", "expert"), None),
            P(("dp", "expert"), None),
            P(("dp", "expert"), None),
            P("expert", "dp", None),
        ),
        out_specs=(P(("dp", "expert"), None), P("expert", "dp", None), P(("dp", "expert"), None)),
        check_vma=False,
    )
```
